32 devices in a mesh: expert: 4 (over y, x), tensor: 4 (over z), dp: 2 (over core).
Axes of the slice: x: 2, y: 2, z: 4, core: 2. Of those that a mesh axis runs over, the one named last changes fastest.
Arguments:
- x_real: bfloat16 [2048, 2048], P(('expert', 'dp'), 'tensor'), may hold values from -6 to 6
- routes_real: int32 [2048, 2], P(('expert', 'dp')), may hold values from 0 to 3, all different within a row; in each aligned block of 256 rows (0 to 255, 256 to 511, ...) at most 128 rows name the same one
- gates_real: float32 [2048, 2], P(('expert', 'dp')), may hold values from 0.2 to 1
- up_real: bfloat16 [4, 2048, 8192], P('expert', None, 'tensor'), may hold values from -0.125 to 0.125
- down_real: bfloat16 [4, 8192, 2048], P('expert', 'tensor'), may hold values from -0.0625 to 0.0625
- x_fake: bfloat16 [2048, 2048], P(('expert', 'dp'), 'tensor'), may hold values from -6 to 6
- routes_fake: int32 [2048, 2], P(('expert', 'dp')), may hold values from 0 to 3, all different within a row; in each aligned block of 256 rows (0 to 255, 256 to 511, ...) at most 128 rows name the same one
- gates_fake: float32 [2048, 2], P(('expert', 'dp')), may hold values from 0.2 to 1
- cotangent: bfloat16 [2048, 2048], P(('expert', 'dp'), 'tensor'), may hold values from -6 to 6
- up_fake: bfloat16 [4, 2048, 8192], P('expert', None, 'tensor'), may hold values from -0.125 to 0.125
- down_fake: bfloat16 [4, 8192, 2048], P('expert', 'tensor'), may hold values from -0.0625 to 0.0625
Outputs:
- real_out: bfloat16 [2048, 2048], P(('expert', 'dp'), 'tensor')
- grad_up: bfloat16 [4, 2048, 8192], P('expert', 'dp', 'tensor')
- grad_down: bfloat16 [4, 8192, 2048], P('expert', 'tensor', 'dp')
The draws below stay inside these ranges and needn't reach their ends.
Inputs may be any that keep to these rules, and one draw needn't show every extreme that they name: `routes_real`: each row names 2 different experts. In the 256 rows of one index of expert and dp no expert is named more than 128 times, and that bound is reached. `routes_fake`: each row names 2 different experts. In the 256 rows of one index of expert and dp no expert is named more than 128 times, and that bound is reached.
All inputs are finite; a program needn't handle non-finite values.
Results may differ from the reference program's by a relative error of at most 0.0058.
Values may be sent and summed in bfloat16 or wider, within the bound.
A program may use at most 192 MiB of HBM per device.

```python
import math
import jax
import jax.numpy as jnp
import numpy as np
from jax import lax

D = 2048
FF = 8192
TOP = 2
TOK_DEV = 256
CAP = 128
EXPERTS = 4
TOKENS = 2048


def block_scale(rng, shape, split, smallest, high):
    loudness = 1.0
    for axis_at, blocks in split:
        draws = jax.random.uniform(jax.random.fold_in(jax.random.fold_in(rng, 6), axis_at), (blocks,), jnp.float32, smallest / len(split), high / len(split))
        loudness = loudness * jnp.repeat(jnp.exp(draws), shape[axis_at] // blocks).reshape((-1,) + (1,) * (len(shape) - 1 - axis_at))
    return loudness


def deal_out(stream_key, own, number, rows, count, top, reach, skew):
    order = jax.random.permutation(stream_key, count)
    crowded, usual = load_shares(count, rows * top, reach, skew, True), load_shares(count, rows * top, reach, skew, False)
    places = jnp.arange(count)

    def named(tallies, turn):
        used = int((tallies > 0).sum())
        fixed = max(1, used // 4)
        shifted = fixed + (places - fixed + turn * (used - fixed)) % max(1, count - fixed)
        return jnp.zeros((count,), jnp.int32).at[order[jnp.where(places < fixed, places, shifted)]].set(jnp.asarray(tallies, jnp.int32))

    tallies = jnp.where(number % 4 == 0, named(crowded, number // 4), named(usual, number - number // 4 - 1))
    mixed = jax.random.permutation(jax.random.fold_in(own, 3), count)
    source_of, receiver = mixed[0:count // 2 * 2:2], mixed[1:count // 2 * 2:2]
    margin = jnp.minimum(tallies[source_of] - 1, reach - tallies[receiver]) // 2
    margin = jnp.where((source_of == order[0]) | (receiver == order[0]) | (tallies[receiver] == 0), 0, jnp.maximum(margin, 0))
    shifted = jax.random.randint(jax.random.fold_in(own, 4), (count // 2,), 0, 1 << 20) % (margin + 1)
    tallies = tallies.at[source_of].add(-shifted).at[receiver].add(shifted)
    members = jnp.searchsorted(jnp.cumsum(tallies), jnp.arange(rows * top), side="right").astype(jnp.int32)
    table = members.reshape(top, rows).T
    table = table[jax.random.permutation(jax.random.fold_in(own, 1), rows)]
    turn = jax.random.randint(jax.random.fold_in(own, 2), (rows, 1), 0, top)
    return jnp.take_along_axis(table, (jnp.arange(top)[None, :] + turn) % top, axis=1)


def load_shares(number_of, total, limit, lean, full):
    weights = [(1 << 20) // math.isqrt(rank ** lean) + 1 for rank in range(1, number_of + 1)]
    largest = limit if full else min(limit, max(-(-total // number_of), total * weights[0] // sum(weights)))
    least = 1 if total - largest >= number_of - 1 else 0
    holding, spare = [largest] + [least] * (number_of - 1), total - largest - least * (number_of - 1)
    while spare > 0:
        free = [i for i in range(1, number_of) if holding[i] < largest] or [i for i in range(1, number_of) if holding[i] < limit]
        mass, left = sum([weights[i] for i in free]), spare
        for i in free:
            addition = min(limit - holding[i], max(1, left * weights[i] // mass), spare)
            holding[i] = holding[i] + addition
            spare = spare - addition
    return np.array(holding)


def scatter_about(rng, extent, deviation, bound, shards=(), kind=jnp.bfloat16):
    array = jax.random.normal(rng, extent, jnp.float32) * deviation
    if len(shards) > 0:
        array = block_scale(rng, extent, shards, -0.22, 0.18) * array
    return jnp.clip(array, min=-bound, max=bound).astype(kind)


def setup_inputs(seed: int = 0) -> dict:
    seeds = jax.random.split(jax.random.key(seed), 12)
    x_real = scatter_about(seeds[0], (TOKENS, D), 1.0, 6.0, ((0, 8), (1, 4)))
    routes_real_keys = jax.random.split(jax.random.fold_in(seeds[1], 1), TOKENS // TOK_DEV)
    routes_real_turns = jax.random.permutation(jax.random.fold_in(seeds[1], 3), TOKENS // TOK_DEV)
    routes_real = jax.vmap(lambda own, number: deal_out(jax.random.fold_in(seeds[1], 2), own, number, TOK_DEV, EXPERTS, TOP, CAP, 2))(routes_real_keys, routes_real_turns).reshape((TOKENS, TOP))
    gates_real = jnp.clip(jnp.exp(math.log(1.0) - 1.609438 * jax.random.uniform(seeds[2], (TOKENS, TOP), jnp.float32) ** block_scale(seeds[2], (TOKENS, TOP), ((0, 8),), -0.2, 0.2)), 0.2, 1.0)
    up_real = scatter_about(seeds[3], (EXPERTS, D, FF), D ** -0.5, 0.125, ((0, 4), (2, 4)))
    down_real = scatter_about(seeds[4], (EXPERTS, FF, D), FF ** -0.5, 0.0625, ((0, 4), (1, 4)))
    x_fake = scatter_about(seeds[5], (TOKENS, D), 1.0, 6.0, ((0, 8), (1, 4)))
    routes_fake_keys = jax.random.split(jax.random.fold_in(seeds[6], 1), TOKENS // TOK_DEV)
    routes_fake_turns = jax.random.permutation(jax.random.fold_in(seeds[6], 3), TOKENS // TOK_DEV)
    routes_fake = jax.vmap(lambda own, number: deal_out(jax.random.fold_in(seeds[6], 2), own, number, TOK_DEV, EXPERTS, TOP, CAP, 2))(routes_fake_keys, routes_fake_turns).reshape((TOKENS, TOP))
    gates_fake = jnp.clip(jnp.exp(math.log(1.0) - 1.609438 * jax.random.uniform(seeds[7], (TOKENS, TOP), jnp.float32) ** block_scale(seeds[7], (TOKENS, TOP), ((0, 8),), -0.2, 0.2)), 0.2, 1.0)
    cotangent = scatter_about(seeds[8], (TOKENS, D), 1.0, 6.0, ((0, 8), (1, 4)))
    up_fake = scatter_about(seeds[9], (EXPERTS, D, FF), D ** -0.5, 0.125, ((0, 4), (2, 4)))
    down_fake = scatter_about(seeds[10], (EXPERTS, FF, D), FF ** -0.5, 0.0625, ((0, 4), (1, 4)))
    return dict(x_real=x_real, routes_real=routes_real, gates_real=gates_real, up_real=up_real, down_real=down_real, x_fake=x_fake, routes_fake=routes_fake, gates_fake=gates_fake, cotangent=cotangent, up_fake=up_fake, down_fake=down_fake)


slope_const = 0.7978845608028654
cubic_coef = 0.044715


def gelu_tanh(value):
    return 0.5 * value * (1.0 + jnp.tanh(slope_const * (value + cubic_coef * value * value * value)))


def gelu_slope(value):
    inner = jnp.tanh(slope_const * (value + cubic_coef * value * value * value))
    return 0.5 * (1.0 + inner) + 0.5 * value * (1.0 - inner * inner) * slope_const * (1.0 + 3.0 * cubic_coef * value * value)


def slot_index(routes):
    blocks = routes.reshape(-1, TOK_DEV, TOP)
    labels = jnp.arange(EXPERTS, dtype=jnp.int32)
    hits = (blocks[:, :, :, None] == labels[None, None, None, :]).astype(jnp.int32)
    per_token = jnp.sum(hits, axis=2)
    before = jnp.cumsum(per_token, axis=1) - per_token
    return jnp.sum(hits * before[:, :, None, :], axis=3).reshape(-1, TOP).astype(jnp.int32)


def block_index():
    column = (jnp.arange(TOKENS, dtype=jnp.int32) // TOK_DEV)[:, None]
    return jnp.broadcast_to(column, (TOKENS, TOP)).astype(jnp.int32)


def to_buffer(rows, routes, slots, block):
    count = TOKENS // TOK_DEV
    width = rows.shape[-1]
    buffer = jnp.zeros((EXPERTS, count, CAP, width), rows.dtype)
    return buffer.at[routes, block, slots].set(rows).reshape(EXPERTS, count * CAP, width)


def reference(x_real, routes_real, gates_real, up_real, down_real, x_fake, routes_fake, gates_fake, cotangent, up_fake, down_fake):
    count = TOKENS // TOK_DEV
    block = block_index()
    slots_real = slot_index(routes_real)
    spread_x = jnp.broadcast_to(x_real[:, None, :], (TOKENS, TOP, D))
    buffer_real = to_buffer(spread_x, routes_real, slots_real, block)

    def run_real(item):
        rows, w_up, w_down = item
        hidden = gelu_tanh(jnp.dot(rows, w_up, preferred_element_type=jnp.float32)).astype(jnp.bfloat16)
        return jnp.dot(hidden, w_down, preferred_element_type=jnp.float32).astype(jnp.bfloat16)

    outputs = lax.map(run_real, (buffer_real, up_real, down_real))
    picked = outputs.reshape(EXPERTS, count, CAP, D)[routes_real, block, slots_real]
    real_out = jnp.sum(gates_real[:, :, None] * picked.astype(jnp.float32), axis=1).astype(jnp.bfloat16)

    slots_fake = slot_index(routes_fake)
    scaled = (gates_fake[:, :, None] * cotangent[:, None, :].astype(jnp.float32)).astype(jnp.bfloat16)
    spread_f = jnp.broadcast_to(x_fake[:, None, :], (TOKENS, TOP, D))
    buffer_x = to_buffer(spread_f, routes_fake, slots_fake, block)
    buffer_d = to_buffer(scaled, routes_fake, slots_fake, block)

    def run_fake(item):
        rows_x, rows_d, w_up, w_down = item
        pre = jnp.dot(rows_x, w_up, preferred_element_type=jnp.float32)
        act = gelu_tanh(pre).astype(jnp.bfloat16)
        back = lax.dot_general(rows_d, w_down, (((1,), (1,)), ((), ())), preferred_element_type=jnp.float32)
        dpre = (back * gelu_slope(pre)).astype(jnp.bfloat16)
        grad_in = lax.dot_general(rows_x, dpre, (((0,), (0,)), ((), ())), preferred_element_type=jnp.float32)
        grad_out = lax.dot_general(act, rows_d, (((0,), (0,)), ((), ())), preferred_element_type=jnp.float32)
        return grad_in.astype(jnp.bfloat16), grad_out.astype(jnp.bfloat16)

    grad_up, grad_down = lax.map(run_fake, (buffer_x, buffer_d, up_fake, down_fake))
    return (real_out, grad_up, grad_down)
```

```python
import functools

import jax
import jax.numpy as jnp
from jax import lax
from jax.experimental import pallas as pl
from jax.experimental.pallas import tpu as pltpu
from jax.sharding import PartitionSpec as P

slope_const = 0.7978845608028654
cubic_coef = 0.044715
MESH = pl.DeviceIdType.MESH
F32 = jnp.float32
BF16 = jnp.bfloat16
LAG = 2


def dot32(left, right, dims=((1,), (0,))):
    return lax.dot_general(left, right, (dims, ((), ())), preferred_element_type=F32)


def tanh_of(value):
    return jnp.tanh(slope_const * (value + cubic_coef * value * value * value))


def gelu_from(value, inner):
    return 0.5 * value * (1.0 + inner)


def slope_from(value, inner):
    return 0.5 * (1.0 + inner) + 0.5 * value * (1.0 - inner * inner) * slope_const * (
        1.0 + 3.0 * cubic_coef * value * value
    )


def moe_kernel(
    experts,
    tensors,
    routes_real,
    gates_real,
    routes_fake,
    gates_fake,
    x_real,
    x_fake,
    cotangent,
    up_real,
    down_real,
    up_fake,
    down_fake,
    real_out,
    grad_up,
    grad_down,
    whole,
    sendbuf,
    rows,
    acc0,
    acc1,
    weight0,
    weight1,
    pick,
    pick_k,
    gate,
    act,
    dpre,
    other_x,
    other_d,
    partial,
    from_left,
    from_right,
    final,
    ret_send,
    returned,
    stage_up,
    stage_down,
    in_sem,
    w_sem,
    z_recv,
    z_right,
    z_left,
    x_send,
    x_recv,
    d_send,
    d_recv,
    big_send,
    big_recv,
    rsr_send,
    rsr_recv,
    rsl_send,
    rsl_recv,
    ret_sems,
    up_sem,
    down_sem,
):
    E, T = experts, tensors
    top, tokens = routes_real.shape
    cap = tokens // 2
    total = E * cap
    part = x_real.shape[1]
    FF = act.shape[1]
    NT = stage_up.shape[2]
    tiles = FF // NT
    half = T // 2
    e = lax.axis_index("expert")
    t = lax.axis_index("tensor")
    d = lax.axis_index("dp")
    last = T - 1

    barrier = pltpu.get_barrier_semaphore()
    for s in range(1, E):
        pl.semaphore_signal(barrier, inc=1, device_id={"expert": e ^ s}, device_id_type=MESH)
    pl.semaphore_signal(barrier, inc=1, device_id={"dp": 1 - d}, device_id_type=MESH)

    @pl.when(t > 0)
    def _():
        pl.semaphore_signal(barrier, inc=1, device_id={"tensor": t - 1}, device_id_type=MESH)

    @pl.when(t < last)
    def _():
        pl.semaphore_signal(barrier, inc=1, device_id={"tensor": t + 1}, device_id_type=MESH)

    own_in = [
        pltpu.make_async_copy(src, whole.at[a * T + t], in_sem.at[a])
        for a, src in enumerate((x_real, x_fake, cotangent))
    ]
    for copy in own_in:
        copy.start()

    def load(src, dst, k):
        return pltpu.make_async_copy(src.at[0], dst, w_sem.at[k])

    load(up_real, weight0, 0).start()
    load(down_real, weight1, 1).start()

    pl.semaphore_wait(barrier, E + jnp.minimum(t, 1) + jnp.minimum(last - t, 1))

    def z_copy(i, q, right):
        a = i // T
        k = a * T + q
        return pltpu.make_async_remote_copy(
            src_ref=whole.at[k],
            dst_ref=whole.at[k],
            send_sem=(z_right if right else z_left).at[k],
            recv_sem=z_recv.at[k],
            device_id={"tensor": t + 1 if right else t - 1},
            device_id_type=MESH,
        )

    near = jnp.minimum(t, last - t)

    def source(p):
        step = (p + 1) // 2
        close = jnp.where(p % 2 == 1, t - step, t + step)
        beyond = jnp.where(t < last - t, t + p - near, t - p + near)
        return jnp.where(p <= 2 * near, close, beyond)

    def gather_step(i):
        q = source(i % T)

        @pl.when(q != t)
        def _():
            z_copy(i, q, True).wait_recv()

        @pl.when(jnp.logical_and(q <= t, t < last))
        def _():
            z_copy(i, q, True).start()

        @pl.when(jnp.logical_and(q >= t, t > 0))
        def _():
            z_copy(i, q, False).start()

    def x_copies(k):
        return [
            pltpu.make_async_remote_copy(
                src_ref=sendbuf.at[k, pl.ds((s - 1) * cap, cap)],
                dst_ref=rows.at[k, pl.ds(s * cap, cap)],
                send_sem=x_send.at[k],
                recv_sem=x_recv.at[k],
                device_id={"expert": e ^ s},
                device_id_type=MESH,
            )
            for s in range(1, E)
        ]

    def x_all(k):
        return pltpu.make_async_remote_copy(
            src_ref=sendbuf.at[k],
            dst_ref=rows.at[k, pl.ds(cap, total - cap)],
            send_sem=x_send.at[k],
            recv_sem=x_recv.at[k],
            device_id={"expert": e ^ 1},
            device_id_type=MESH,
        )

    def dispatch_step(i):
        a = i // T
        k = a * T + source(i % T)
        which = jnp.minimum(a, 1)
        picked = (dot32(pick[which], whole[k]) * gate[a]).astype(BF16)
        rows[k, 0:cap] = picked[0:cap]
        sendbuf[k] = picked[cap:total]
        for copy in x_copies(k):
            copy.start()

    def feed(i):
        gather_step(i)
        dispatch_step(i)

    own_in[0].wait()
    gather_step(0)

    square = (tokens, tokens)
    down_at = lax.broadcasted_iota(jnp.int32, square, 0)
    along = lax.broadcasted_iota(jnp.int32, square, 1)
    eye = down_at == along
    upper = (down_at < along).astype(BF16)
    labels_high = max(8, E)
    labels = lax.broadcasted_iota(jnp.int32, (labels_high, tokens), 0).astype(F32)
    slot_rows = lax.broadcasted_iota(jnp.int32, (total, tokens), 0).astype(F32)

    def stand_up(row):
        return jnp.sum(jnp.where(eye, row, 0.0), axis=1, keepdims=True)

    def positions(routes):
        names = [routes[k : k + 1, :].astype(F32) for k in range(top)]
        places = [(routes[k : k + 1, :] ^ e).astype(F32) for k in range(top)]
        hits = jnp.zeros((labels_high, tokens), F32)
        for name in names:
            hits = hits + (labels == name).astype(F32)
        before = dot32(hits.astype(BF16), upper)
        found = []
        for name, place in zip(names, places):
            slot = jnp.sum(jnp.where(labels == name, before, 0.0), axis=0, keepdims=True)
            found.append(place * cap + slot)
        return found

    chosen = jnp.zeros((total, tokens), BF16)
    for k, where in enumerate(positions(routes_real)):
        mask = (slot_rows == where).astype(F32).astype(BF16)
        pick_k[k] = mask
        chosen = chosen + mask
    pick[0] = chosen
    gate[0] = jnp.ones((total, 1), F32)
    dispatch_step(0)
    gate[1] = jnp.ones((total, 1), F32)
    chosen = jnp.zeros((total, tokens), BF16)
    gated = jnp.zeros((total, tokens), F32)
    for k, where in enumerate(positions(routes_fake)):
        mask = slot_rows == where
        chosen = chosen + mask.astype(F32).astype(BF16)
        gated = jnp.where(mask, gates_fake[k : k + 1, :], gated)
    pick[1] = chosen
    gate[2] = jnp.sum(gated, axis=1, keepdims=True)
    own_in[1].wait()
    own_in[2].wait()
    for i in range(1, LAG):
        feed(jnp.int32(i))

    def tile_at(n):
        return pl.ds(pl.multiple_of(n * NT, NT), NT)

    def part_at(q):
        return pl.ds(pl.multiple_of(q * part, part), part)

    def clear(target):
        @pl.loop(0, tiles)
        def _(n):
            target[:, tile_at(n)] = jnp.zeros((total, NT), F32)

    clear(acc0)
    load(up_real, weight0, 0).wait()

    @pl.loop(0, T)
    def _(p):
        q = source(p)
        x_all(q).wait_recv()

        @pl.loop(0, tiles)
        def _(n):
            acc0[:, tile_at(n)] += dot32(rows[q], weight0[part_at(q), tile_at(n)])

        feed(p + LAG)

    load(up_fake, weight0, 2).start()

    @pl.loop(0, tiles)
    def _(n):
        value = acc0[:, tile_at(n)]
        dpre[0:total, tile_at(n)] = gelu_from(value, tanh_of(value)).astype(BF16)

    load(down_real, weight1, 1).wait()

    @pl.loop(0, T)
    def _(c):
        partial[c] = dot32(dpre[0:total], weight1[:, part_at(c)]).astype(BF16)

    load(down_fake, weight1, 3).start()

    def rs_right(c, first):
        return pltpu.make_async_remote_copy(
            src_ref=partial.at[c] if first else from_left.at[c],
            dst_ref=from_left.at[c],
            send_sem=rsr_send.at[c],
            recv_sem=rsr_recv.at[c],
            device_id={"tensor": t + 1},
            device_id_type=MESH,
        )

    def rs_left(c, first):
        return pltpu.make_async_remote_copy(
            src_ref=partial.at[c] if first else from_right.at[c],
            dst_ref=from_right.at[c],
            send_sem=rsl_send.at[c],
            recv_sem=rsl_recv.at[c],
            device_id={"tensor": t - 1},
            device_id_type=MESH,
        )

    def rs_round(h):
        c_right = last - h + t
        go_right = jnp.logical_and(h >= t, t < last)

        @pl.when(jnp.logical_and(go_right, t == 0))
        def _():
            rs_right(c_right, True).start()

        @pl.when(jnp.logical_and(go_right, t > 0))
        def _():
            rs_right(c_right, False).wait_recv()
            joined = from_left[c_right].astype(F32) + partial[c_right].astype(F32)
            from_left[c_right] = joined.astype(BF16)
            rs_right(c_right, False).start()

        c_left = h - (last - t)
        go_left = jnp.logical_and(h >= last - t, t > 0)

        @pl.when(jnp.logical_and(go_left, t == last))
        def _():
            rs_left(c_left, True).start()

        @pl.when(jnp.logical_and(go_left, t < last))
        def _():
            rs_left(c_left, False).wait_recv()
            joined = from_right[c_left].astype(F32) + partial[c_left].astype(F32)
            from_right[c_left] = joined.astype(BF16)
            rs_left(c_left, False).start()

    def ret_copies():
        return [
            pltpu.make_async_remote_copy(
                src_ref=ret_send.at[pl.ds(s * cap, cap)],
                dst_ref=returned.at[pl.ds(s * cap, cap)],
                send_sem=ret_sems.at[0],
                recv_sem=ret_sems.at[1],
                device_id={"expert": e ^ s},
                device_id_type=MESH,
            )
            for s in range(1, E)
        ]

    def ret_all():
        return pltpu.make_async_remote_copy(
            src_ref=ret_send.at[pl.ds(cap, total - cap)],
            dst_ref=returned.at[pl.ds(cap, total - cap)],
            send_sem=ret_sems.at[0],
            recv_sem=ret_sems.at[1],
            device_id={"expert": e ^ 1},
            device_id_type=MESH,
        )

    def rs_final():
        final[...] = partial[t].astype(F32)

        @pl.when(t > 0)
        def _():
            rs_right(t, False).wait_recv()
            final[...] += from_left[t].astype(F32)

        @pl.when(t < last)
        def _():
            rs_left(t, False).wait_recv()
            final[...] += from_right[t].astype(F32)

        summed = final[...].astype(BF16)
        ret_send[...] = summed
        returned[0:cap] = summed[0:cap]
        for copy in ret_copies():
            copy.start()

    def rs_slot(j):
        h = j // 2

        @pl.when(jnp.logical_and(j % 2 == 0, jnp.logical_and(j > 0, h < last)))
        def _():
            rs_round(h)

        @pl.when(j == 2 * last)
        def _():
            rs_final()

    rs_round(jnp.int32(0))

    def half_of(q):
        return q // half

    def swap(a, q, target):
        k = a * T + q
        other = q - (1 - d) * half
        return pltpu.make_async_remote_copy(
            src_ref=rows.at[k],
            dst_ref=target.at[other],
            send_sem=d_send.at[(a - 1) * half + other],
            recv_sem=d_recv.at[(a - 1) * half + other],
            device_id={"dp": 1 - d},
            device_id_type=MESH,
        )

    clear(acc1)
    load(up_fake, weight0, 2).wait()

    @pl.loop(0, T)
    def _(p):
        q = source(p)
        x_all(T + q).wait_recv()

        @pl.when(half_of(q) != d)
        def _():
            swap(1, q, other_x).start()

        @pl.loop(0, tiles)
        def _(n):
            acc1[:, tile_at(n)] += dot32(rows[T + q], weight0[part_at(q), tile_at(n)])

        feed(T + p + LAG)
        rs_slot(p)

    @pl.loop(0, tiles)
    def _(n):
        value = acc1[:, tile_at(n)]
        inner = tanh_of(value)
        act[0:total, tile_at(n)] = gelu_from(value, inner).astype(BF16)
        acc1[:, tile_at(n)] = slope_from(value, inner)

    def across(buffer, k):
        return pltpu.make_async_remote_copy(
            src_ref=buffer.at[pl.ds(0, total)],
            dst_ref=buffer.at[pl.ds(total, total)],
            send_sem=big_send.at[k],
            recv_sem=big_recv.at[k],
            device_id={"dp": 1 - d},
            device_id_type=MESH,
        )

    clear(acc0)
    across(act, 0).start()
    load(down_fake, weight1, 3).wait()

    @pl.loop(0, T)
    def _(p):
        q = source(p)
        x_all(2 * T + q).wait_recv()

        @pl.when(half_of(q) != d)
        def _():
            swap(2, q, other_d).start()

        @pl.loop(0, tiles)
        def _(n):
            acc0[:, tile_at(n)] += dot32(
                rows[2 * T + q], weight1[tile_at(n), part_at(q)], ((1,), (1,))
            )

        @pl.when(p + LAG < T)
        def _():
            feed(2 * T + p + LAG)

        rs_slot(T + p)

    @pl.loop(0, tiles)
    def _(n):
        dpre[0:total, tile_at(n)] = (acc0[:, tile_at(n)] * acc1[:, tile_at(n)]).astype(BF16)

    across(dpre, 1).start()

    def other_in(a, j, target):
        return pltpu.make_async_remote_copy(
            src_ref=rows.at[a * T + j],
            dst_ref=target.at[j],
            send_sem=d_send.at[(a - 1) * half + j],
            recv_sem=d_recv.at[(a - 1) * half + j],
            device_id={"dp": 1 - d},
            device_id_type=MESH,
        )

    @pl.loop(0, half)
    def _(j):
        other_in(1, j, other_x).wait_recv()
        other_in(2, j, other_d).wait_recv()

    across(act, 0).wait_recv()
    base = d * half

    def put_down(j, n):
        slot = (j * tiles + n) % 2
        return pltpu.make_async_copy(
            stage_down.at[slot], grad_down.at[0, tile_at(n), part_at(j)], down_sem.at[slot]
        )

    def put_up(j, n):
        slot = (j * tiles + n) % 2
        return pltpu.make_async_copy(
            stage_up.at[slot], grad_up.at[0, part_at(j), tile_at(n)], up_sem.at[slot]
        )

    @pl.loop(0, half * tiles)
    def _(w):
        j = w // tiles
        n = w % tiles

        @pl.when(w >= 2)
        def _():
            put_down(j, n).wait()

        tile = dot32(act[0:total, tile_at(n)], rows[2 * T + base + j], ((0,), (0,)))
        tile = tile + dot32(act[total : 2 * total, tile_at(n)], other_d[j], ((0,), (0,)))
        stage_down[w % 2] = tile.astype(BF16)
        put_down(j, n).start()

    across(dpre, 1).wait_recv()

    @pl.loop(0, half * tiles)
    def _(w):
        j = w // tiles
        n = w % tiles

        @pl.when(w >= 2)
        def _():
            put_up(j, n).wait()

        tile = dot32(rows[T + base + j], dpre[0:total, tile_at(n)], ((0,), (0,)))
        tile = tile + dot32(other_x[j], dpre[total : 2 * total, tile_at(n)], ((0,), (0,)))
        stage_up[w % 2] = tile.astype(BF16)
        put_up(j, n).start()

    ret_all().wait_recv()
    out = jnp.zeros((tokens, part), F32)
    for k in range(top):
        back = dot32(pick_k[k], returned[...], ((0,), (0,)))
        out = out + stand_up(gates_real[k : k + 1, :]) * back
    real_out[...] = out.astype(BF16)

    for w in range(max(0, half * tiles - 2), half * tiles):
        put_down(w // tiles, w % tiles).wait()
        put_up(w // tiles, w % tiles).wait()

    @pl.loop(0, 3 * T)
    def _(k):
        x_all(k).wait_send()
        q = k % T

        @pl.when(jnp.logical_and(q <= t, t < last))
        def _():
            z_copy(k, q, True).wait_send()

        @pl.when(jnp.logical_and(q >= t, t > 0))
        def _():
            z_copy(k, q, False).wait_send()

    @pl.loop(0, half)
    def _(j):
        other_in(1, j, other_x).wait_send()
        other_in(2, j, other_d).wait_send()

    across(act, 0).wait_send()
    across(dpre, 1).wait_send()
    ret_all().wait_send()

    @pl.loop(0, T)
    def _(c):
        @pl.when(c > t)
        def _():
            rs_right(c, False).wait_send()

        @pl.when(c < t)
        def _():
            rs_left(c, False).wait_send()


def on_device(
    x_real,
    routes_real,
    gates_real,
    up_real,
    down_real,
    x_fake,
    routes_fake,
    gates_fake,
    cotangent,
    up_fake,
    down_fake,
):
    E = lax.axis_size("expert")
    T = lax.axis_size("tensor")
    tokens, part = x_real.shape
    top = routes_real.shape[1]
    cap = tokens // 2
    total = E * cap
    D = up_real.shape[1]
    FF = up_real.shape[2]
    NT = min(512, FF)
    half = T // 2
    vmem = pl.BlockSpec(memory_space=pltpu.VMEM)
    hbm = pl.BlockSpec(memory_space=pl.ANY)
    dma = pltpu.SemaphoreType.DMA
    return pl.pallas_call(
        functools.partial(moe_kernel, E, T),
        name="moe",
        out_shape=(
            jax.ShapeDtypeStruct((tokens, part), BF16),
            jax.ShapeDtypeStruct((1, D // 2, FF), BF16),
            jax.ShapeDtypeStruct((1, FF, D // 2), BF16),
        ),
        in_specs=[vmem] * 4 + [hbm] * 7,
        out_specs=(vmem, hbm, hbm),
        scratch_shapes=[
            pltpu.VMEM((3 * T, tokens, part), BF16),
            pltpu.VMEM((3 * T, total - cap, part), BF16),
            pltpu.VMEM((3 * T, total, part), BF16),
            pltpu.VMEM((total, FF), F32),
            pltpu.VMEM((total, FF), F32),
            pltpu.VMEM((D, FF), BF16),
            pltpu.VMEM((FF, D), BF16),
            pltpu.VMEM((2, total, tokens), BF16),
            pltpu.VMEM((top, total, tokens), BF16),
            pltpu.VMEM((3, total, 1), F32),
            pltpu.VMEM((2 * total, FF), BF16),
            pltpu.VMEM((2 * total, FF), BF16),
            pltpu.VMEM((half, total, part), BF16),
            pltpu.VMEM((half, total, part), BF16),
            pltpu.VMEM((T, total, part), BF16),
            pltpu.VMEM((T, total, part), BF16),
            pltpu.VMEM((T, total, part), BF16),
            pltpu.VMEM((total, part), F32),
            pltpu.VMEM((total, part), BF16),
            pltpu.VMEM((total, part), BF16),
            pltpu.VMEM((2, part, NT), BF16),
            pltpu.VMEM((2, NT, part), BF16),
            dma((3,)),
            dma((4,)),
            dma((3 * T,)),
            dma((3 * T,)),
            dma((3 * T,)),
            dma((3 * T,)),
            dma((3 * T,)),
            dma((2 * half,)),
            dma((2 * half,)),
            dma((2,)),
            dma((2,)),
            dma((T,)),
            dma((T,)),
            dma((T,)),
            dma((T,)),
            dma((2,)),
            dma((2,)),
            dma((2,)),
        ],
        compiler_params=pltpu.CompilerParams(
            collective_id=0, has_side_effects=True, vmem_limit_bytes=67043328
        ),
    )(
        routes_real.T,
        gates_real.T,
        routes_fake.T,
        gates_fake.T,
        x_real,
        x_fake,
        cotangent,
        up_real,
        down_real,
        up_fake,
        down_fake,
    )


def solution(mesh):
    in_specs = (
        P(("expert", "dp"), "tensor"),
        P(("expert", "dp"), None),
        P(("expert", "dp"), None),
        P("expert", None, "tensor"),
        P("expert", "tensor", None),
        P(("expert", "dp"), "tensor"),
        P(("expert", "dp"), None),
        P(("expert", "dp"), None),
        P(("expert", "dp"), "tensor"),
        P("expert", None, "tensor"),
        P("expert", "tensor", None),
    )
    out_specs = (
        P(("expert", "dp"), "tensor"),
        P("expert", "dp", "tensor"),
        P("expert", "tensor", "dp"),
    )
    return jax.shard_map(
        on_device, mesh=mesh, in_specs=in_specs, out_specs=out_specs, check_vma=False
    )
```

```python
import functools

import jax
import jax.numpy as jnp
from jax import lax
from jax.experimental import pallas as pl
from jax.experimental.pallas import tpu as pltpu
from jax.sharding import PartitionSpec as P

slope_const = 0.7978845608028654
cubic_coef = 0.044715
MESH = pl.DeviceIdType.MESH
F32 = jnp.float32
BF16 = jnp.bfloat16
LAG = 3
CUTS = 2


def dot32(left, right, dims=((1,), (0,))):
    return lax.dot_general(left, right, (dims, ((), ())), preferred_element_type=F32)


def tanh_of(value):
    return jnp.tanh(slope_const * (value + cubic_coef * value * value * value))


def gelu_from(value, inner):
    return 0.5 * value * (1.0 + inner)


def slope_from(value, inner):
    return 0.5 * (1.0 + inner) + 0.5 * value * (1.0 - inner * inner) * slope_const * (
        1.0 + 3.0 * cubic_coef * value * value
    )


def moe_kernel(
    experts,
    tensors,
    routes_real,
    gates_real,
    routes_fake,
    gates_fake,
    x_real,
    x_fake,
    cotangent,
    up_real,
    down_real,
    up_fake,
    down_fake,
    real_out,
    x_up,
    d_up,
    grad_down,
    whole,
    sendbuf,
    rows,
    acc0,
    acc1,
    weight0,
    weight1,
    pick,
    pick_k,
    gate,
    act,
    dpre,
    x_turned,
    other_d,
    partial,
    from_left,
    from_right,
    final,
    ret_send,
    returned,
    stage_down,
    in_sem,
    w_sem,
    z_recv,
    z_right,
    z_left,
    x_send,
    x_recv,
    xt_keep,
    xt_send,
    xt_recv,
    d_send,
    d_recv,
    act_sems,
    dp_keep,
    dp_send,
    dp_recv,
    rsr_send,
    rsr_recv,
    rsl_send,
    rsl_recv,
    ret_sems,
    down_sem,
):
    E, T = experts, tensors
    top, tokens = routes_real.shape
    cap = tokens // 2
    total = E * cap
    part = x_real.shape[1]
    FF = act.shape[1]
    NT = stage_down.shape[1]
    tiles = FF // NT
    half = T // 2
    e = lax.axis_index("expert")
    t = lax.axis_index("tensor")
    d = lax.axis_index("dp")
    last = T - 1

    barrier = pltpu.get_barrier_semaphore()
    for s in range(1, E):
        pl.semaphore_signal(barrier, inc=1, device_id={"expert": e ^ s}, device_id_type=MESH)
    pl.semaphore_signal(barrier, inc=1, device_id={"dp": 1 - d}, device_id_type=MESH)

    @pl.when(t > 0)
    def _():
        pl.semaphore_signal(barrier, inc=1, device_id={"tensor": t - 1}, device_id_type=MESH)

    @pl.when(t < last)
    def _():
        pl.semaphore_signal(barrier, inc=1, device_id={"tensor": t + 1}, device_id_type=MESH)

    own_in = [
        pltpu.make_async_copy(src, whole.at[a * T + t], in_sem.at[a])
        for a, src in enumerate((x_real, x_fake, cotangent))
    ]
    for copy in own_in:
        copy.start()

    def load(src, dst, k):
        return pltpu.make_async_copy(src.at[0], dst, w_sem.at[k])

    pl.semaphore_wait(barrier, E + jnp.minimum(t, 1) + jnp.minimum(last - t, 1))

    piece = tokens // CUTS

    def z_copy(i, q, cut, right):
        k = (i // T) * T + q
        return pltpu.make_async_remote_copy(
            src_ref=whole.at[k, pl.ds(cut * piece, piece)],
            dst_ref=whole.at[k, pl.ds(cut * piece, piece)],
            send_sem=(z_right if right else z_left).at[k, cut],
            recv_sem=z_recv.at[k, cut],
            device_id={"tensor": t + 1 if right else t - 1},
            device_id_type=MESH,
        )

    near = jnp.minimum(t, last - t)

    def source(p):
        step = (p + 1) // 2
        close = jnp.where(p % 2 == 1, t - step, t + step)
        beyond = jnp.where(t < last - t, t + p - near, t - p + near)
        return jnp.where(p <= 2 * near, close, beyond)

    at_end = jnp.logical_or(t == 0, t == last)

    def send_own(i):
        for cut in range(CUTS):

            @pl.when(t < last)
            def _():
                z_copy(i, t, cut, True).start()

            @pl.when(t > 0)
            def _():
                z_copy(i, t, cut, False).start()

    def gather_step(i):
        q = source(i % T)

        @pl.when(jnp.logical_and(q == t, jnp.logical_not(at_end)))
        def _():
            send_own(i)

        for cut in range(CUTS):

            @pl.when(q != t)
            def _():
                z_copy(i, q, cut, True).wait_recv()

            @pl.when(jnp.logical_and(q < t, t < last))
            def _():
                z_copy(i, q, cut, True).start()

            @pl.when(jnp.logical_and(q > t, t > 0))
            def _():
                z_copy(i, q, cut, False).start()

    def x_copies(k):
        return [
            pltpu.make_async_remote_copy(
                src_ref=sendbuf.at[k, pl.ds((s - 1) * cap, cap)],
                dst_ref=rows.at[k, pl.ds(s * cap, cap)],
                send_sem=x_send.at[k],
                recv_sem=x_recv.at[k],
                device_id={"expert": e ^ s},
                device_id_type=MESH,
            )
            for s in range(1, E)
        ]

    def x_all(k):
        return pltpu.make_async_remote_copy(
            src_ref=sendbuf.at[k],
            dst_ref=rows.at[k, pl.ds(cap, total - cap)],
            send_sem=x_send.at[k],
            recv_sem=x_recv.at[k],
            device_id={"expert": e ^ 1},
            device_id_type=MESH,
        )

    def dispatch_step(i):
        a = i // T
        k = a * T + source(i % T)
        which = jnp.minimum(a, 1)
        picked = (dot32(pick[which], whole[k]) * gate[a]).astype(BF16)
        rows[k, 0:cap] = picked[0:cap]
        sendbuf[k] = picked[cap:total]
        for copy in x_copies(k):
            copy.start()

    inner = jnp.logical_not(at_end)

    def feed(i):
        @pl.when(at_end)
        def _():
            gather_step(i)

        dispatch_step(i)

    own_in[0].wait()
    send_own(0)
    own_in[1].wait()
    own_in[2].wait()

    @pl.when(at_end)
    def _():
        send_own(T)
        send_own(2 * T)

    load(up_real, weight0, 0).start()

    square = (tokens, tokens)
    down_at = lax.broadcasted_iota(jnp.int32, square, 0)
    along = lax.broadcasted_iota(jnp.int32, square, 1)
    eye = down_at == along
    upper = (down_at < along).astype(BF16)
    labels_high = max(8, E)
    labels = lax.broadcasted_iota(jnp.int32, (labels_high, tokens), 0).astype(F32)
    slot_rows = lax.broadcasted_iota(jnp.int32, (total, tokens), 0).astype(F32)

    def stand_up(row):
        return jnp.sum(jnp.where(eye, row, 0.0), axis=1, keepdims=True)

    def positions(routes):
        names = [routes[k : k + 1, :].astype(F32) for k in range(top)]
        places = [(routes[k : k + 1, :] ^ e).astype(F32) for k in range(top)]
        hits = jnp.zeros((labels_high, tokens), F32)
        for name in names:
            hits = hits + (labels == name).astype(F32)
        before = dot32(hits.astype(BF16), upper)
        found = []
        for name, place in zip(names, places):
            slot = jnp.sum(jnp.where(labels == name, before, 0.0), axis=0, keepdims=True)
            found.append(place * cap + slot)
        return found

    chosen = jnp.zeros((total, tokens), BF16)
    for k, where in enumerate(positions(routes_real)):
        mask = (slot_rows == where).astype(F32).astype(BF16)
        pick_k[k] = mask
        chosen = chosen + mask
    pick[0] = chosen
    gate[0] = jnp.ones((total, 1), F32)
    dispatch_step(0)
    gate[1] = jnp.ones((total, 1), F32)
    chosen = jnp.zeros((total, tokens), BF16)
    gated = jnp.zeros((total, tokens), F32)
    for k, where in enumerate(positions(routes_fake)):
        mask = slot_rows == where
        chosen = chosen + mask.astype(F32).astype(BF16)
        gated = jnp.where(mask, gates_fake[k : k + 1, :], gated)
    pick[1] = chosen
    gate[2] = jnp.sum(gated, axis=1, keepdims=True)
    for i in range(1, LAG):
        gather_step(jnp.int32(i))
        dispatch_step(jnp.int32(i))

    @pl.when(inner)
    def _():
        gather_step(jnp.int32(LAG))


    def tile_at(n):
        return pl.ds(pl.multiple_of(n * NT, NT), NT)

    def part_at(q):
        return pl.ds(pl.multiple_of(q * part, part), part)

    def clear(target):
        @pl.loop(0, tiles)
        def _(n):
            target[:, tile_at(n)] = jnp.zeros((total, NT), F32)

    clear(acc0)
    load(down_real, weight1, 1).start()
    load(up_real, weight0, 0).wait()

    @pl.loop(0, T)
    def _(p):
        q = source(p)
        x_all(q).wait_recv()

        @pl.loop(0, tiles)
        def _(n):
            acc0[:, tile_at(n)] += dot32(rows[q], weight0[part_at(q), tile_at(n)])

        feed(p + LAG)

        @pl.when(inner)
        def _():
            gather_step(p + LAG + 1)

    load(up_fake, weight0, 2).start()

    @pl.loop(0, tiles)
    def _(n):
        value = acc0[:, tile_at(n)]
        dpre[:, tile_at(n)] = gelu_from(value, tanh_of(value)).astype(BF16)

    def rs_right(c, first):
        return pltpu.make_async_remote_copy(
            src_ref=partial.at[c] if first else from_left.at[c],
            dst_ref=from_left.at[c],
            send_sem=rsr_send.at[c],
            recv_sem=rsr_recv.at[c],
            device_id={"tensor": t + 1},
            device_id_type=MESH,
        )

    def rs_left(c, first):
        return pltpu.make_async_remote_copy(
            src_ref=partial.at[c] if first else from_right.at[c],
            dst_ref=from_right.at[c],
            send_sem=rsl_send.at[c],
            recv_sem=rsl_recv.at[c],
            device_id={"tensor": t - 1},
            device_id_type=MESH,
        )

    def rs_round(h):
        c_right = last - h + t
        go_right = jnp.logical_and(h >= t, t < last)

        @pl.when(jnp.logical_and(go_right, t == 0))
        def _():
            rs_right(c_right, True).start()

        @pl.when(jnp.logical_and(go_right, t > 0))
        def _():
            rs_right(c_right, False).wait_recv()
            joined = from_left[c_right].astype(F32) + partial[c_right].astype(F32)
            from_left[c_right] = joined.astype(BF16)
            rs_right(c_right, False).start()

        c_left = h - (last - t)
        go_left = jnp.logical_and(h >= last - t, t > 0)

        @pl.when(jnp.logical_and(go_left, t == last))
        def _():
            rs_left(c_left, True).start()

        @pl.when(jnp.logical_and(go_left, t < last))
        def _():
            rs_left(c_left, False).wait_recv()
            joined = from_right[c_left].astype(F32) + partial[c_left].astype(F32)
            from_right[c_left] = joined.astype(BF16)
            rs_left(c_left, False).start()

    def ret_copies():
        return [
            pltpu.make_async_remote_copy(
                src_ref=ret_send.at[pl.ds(s * cap, cap)],
                dst_ref=returned.at[pl.ds(s * cap, cap)],
                send_sem=ret_sems.at[0],
                recv_sem=ret_sems.at[1],
                device_id={"expert": e ^ s},
                device_id_type=MESH,
            )
            for s in range(1, E)
        ]

    def ret_all():
        return pltpu.make_async_remote_copy(
            src_ref=ret_send.at[pl.ds(cap, total - cap)],
            dst_ref=returned.at[pl.ds(cap, total - cap)],
            send_sem=ret_sems.at[0],
            recv_sem=ret_sems.at[1],
            device_id={"expert": e ^ 1},
            device_id_type=MESH,
        )

    def rs_final():
        final[...] = partial[t].astype(F32)

        @pl.when(t > 0)
        def _():
            rs_right(t, False).wait_recv()
            final[...] += from_left[t].astype(F32)

        @pl.when(t < last)
        def _():
            rs_left(t, False).wait_recv()
            final[...] += from_right[t].astype(F32)

        summed = final[...].astype(BF16)
        ret_send[...] = summed
        returned[0:cap] = summed[0:cap]
        for copy in ret_copies():
            copy.start()

    def rs_slot(j):
        h = j // 2

        @pl.when(jnp.logical_and(j % 2 == 0, jnp.logical_and(j > 0, h < last)))
        def _():
            rs_round(h)

        @pl.when(j == 2 * last + 1)
        def _():
            rs_final()

    load(down_real, weight1, 1).wait()

    @pl.loop(0, T)
    def _(k):
        c = jnp.where(t < half, last - k, k)
        partial[c] = dot32(dpre[...], weight1[:, part_at(c)]).astype(BF16)

        @pl.when(k == 0)
        def _():
            rs_round(jnp.int32(0))

        @pl.when(jnp.logical_and(inner, k < 2))
        def _():
            gather_step(T + LAG + 1 + k)

    load(down_fake, weight1, 3).start()

    def half_of(q):
        return q // half

    base = d * half

    def swap(q):
        other = q - (1 - d) * half
        return pltpu.make_async_remote_copy(
            src_ref=rows.at[2 * T + q],
            dst_ref=other_d.at[other],
            send_sem=d_send.at[other],
            recv_sem=d_recv.at[other],
            device_id={"dp": 1 - d},
            device_id_type=MESH,
        )

    def swap_in(j):
        return pltpu.make_async_remote_copy(
            src_ref=rows.at[2 * T + j],
            dst_ref=other_d.at[j],
            send_sem=d_send.at[j],
            recv_sem=d_recv.at[j],
            device_id={"dp": 1 - d},
            device_id_type=MESH,
        )

    def turned_keep(q):
        return pltpu.make_async_copy(
            x_turned.at[q],
            x_up.at[pl.ds((q - base) * part, part), pl.ds(0, total)],
            xt_keep.at[q - base],
        )

    def turned_send(q):
        other = q - (1 - d) * half
        return pltpu.make_async_remote_copy(
            src_ref=x_turned.at[q],
            dst_ref=x_up.at[pl.ds(other * part, part), pl.ds(total, total)],
            send_sem=xt_send.at[other],
            recv_sem=xt_recv.at[other],
            device_id={"dp": 1 - d},
            device_id_type=MESH,
        )

    def turned_in(j):
        return pltpu.make_async_remote_copy(
            src_ref=x_turned.at[j],
            dst_ref=x_up.at[pl.ds(j * part, part), pl.ds(total, total)],
            send_sem=xt_send.at[j],
            recv_sem=xt_recv.at[j],
            device_id={"dp": 1 - d},
            device_id_type=MESH,
        )

    clear(acc1)
    load(up_fake, weight0, 2).wait()

    @pl.loop(0, T)
    def _(p):
        q = source(p)
        x_all(T + q).wait_recv()

        @pl.loop(0, tiles)
        def _(n):
            acc1[:, tile_at(n)] += dot32(rows[T + q], weight0[part_at(q), tile_at(n)])

        feed(T + p + LAG)
        rs_slot(p)

        @pl.when(jnp.logical_and(inner, p + LAG + 3 < 2 * T))
        def _():
            gather_step(T + p + LAG + 3)

        x_turned[q] = rows[T + q].T

        @pl.when(half_of(q) == d)
        def _():
            turned_keep(q).start()

        @pl.when(half_of(q) != d)
        def _():
            turned_send(q).start()

    @pl.loop(0, tiles)
    def _(n):
        value = acc1[:, tile_at(n)]
        inner = tanh_of(value)
        act[0:total, tile_at(n)] = gelu_from(value, inner).astype(BF16)
        acc1[:, tile_at(n)] = slope_from(value, inner)

    def act_across():
        return pltpu.make_async_remote_copy(
            src_ref=act.at[pl.ds(0, total)],
            dst_ref=act.at[pl.ds(total, total)],
            send_sem=act_sems.at[0],
            recv_sem=act_sems.at[1],
            device_id={"dp": 1 - d},
            device_id_type=MESH,
        )

    def dpre_keep(n):
        return pltpu.make_async_copy(
            dpre.at[:, tile_at(n)], d_up.at[pl.ds(0, total), tile_at(n)], dp_keep.at[n]
        )

    def dpre_across(n):
        return pltpu.make_async_remote_copy(
            src_ref=dpre.at[:, tile_at(n)],
            dst_ref=d_up.at[pl.ds(total, total), tile_at(n)],
            send_sem=dp_send.at[n],
            recv_sem=dp_recv.at[n],
            device_id={"dp": 1 - d},
            device_id_type=MESH,
        )

    def put_down(j, n):
        return pltpu.make_async_copy(
            stage_down.at[n], grad_down.at[tile_at(n), part_at(j)], down_sem.at[n]
        )

    first_down = jnp.clip(t, base, base + half - 1)

    def down_step(q):
        @pl.when(half_of(q) == d)
        def _():
            j = q - base
            swap_in(j).wait_recv()

            @pl.loop(0, tiles)
            def _(n):
                @pl.when(q != first_down)
                def _():
                    put_down(j, n).wait()

                tile = dot32(act[0:total, tile_at(n)], rows[2 * T + q], ((0,), (0,)))
                tile = tile + dot32(
                    act[total : 2 * total, tile_at(n)], other_d[j], ((0,), (0,))
                )
                stage_down[n] = tile.astype(BF16)
                put_down(j, n).start()

    clear(acc0)
    act_across().start()
    load(down_fake, weight1, 3).wait()

    def take_rows(q):
        x_all(2 * T + q).wait_recv()

        @pl.when(half_of(q) != d)
        def _():
            swap(q).start()

    @pl.loop(0, last)
    def _(p):
        q = source(p)
        take_rows(q)

        @pl.loop(0, tiles)
        def _(n):
            acc0[:, tile_at(n)] += dot32(
                rows[2 * T + q], weight1[tile_at(n), part_at(q)], ((1,), (1,))
            )

        @pl.when(p + LAG < T)
        def _():
            feed(2 * T + p + LAG)

        @pl.when(jnp.logical_and(inner, p + LAG + 3 < T))
        def _():
            gather_step(2 * T + p + LAG + 3)

        rs_slot(T + p)

        @pl.when(p == 0)
        def _():
            act_across().wait_recv()

        @pl.when(p > 0)
        def _():
            down_step(source(p - 1))

    q_last = source(last)
    take_rows(q_last)

    @pl.loop(0, tiles)
    def _(n):
        back = acc0[:, tile_at(n)] + dot32(
            rows[2 * T + q_last], weight1[tile_at(n), part_at(q_last)], ((1,), (1,))
        )
        dpre[:, tile_at(n)] = (back * acc1[:, tile_at(n)]).astype(BF16)
        dpre_across(n).start()
        dpre_keep(n).start()

    rs_slot(T + last)
    down_step(source(last - 1))
    down_step(q_last)

    ret_all().wait_recv()
    out = jnp.zeros((tokens, part), F32)
    for k in range(top):
        back = dot32(pick_k[k], returned[...], ((0,), (0,)))
        out = out + stand_up(gates_real[k : k + 1, :]) * back
    real_out[...] = out.astype(BF16)

    @pl.loop(0, tiles)
    def _(n):
        put_down(0, n).wait()
        dpre_across(n).wait()
        dpre_keep(n).wait()

    @pl.loop(0, half)
    def _(j):
        turned_in(j).wait()
        turned_keep(base + j).wait()
        swap_in(j).wait_send()

    act_across().wait_send()

    @pl.loop(0, 3 * T)
    def _(k):
        x_all(k).wait_send()
        q = k % T
        for cut in range(CUTS):

            @pl.when(jnp.logical_and(q <= t, t < last))
            def _():
                z_copy(k, q, cut, True).wait_send()

            @pl.when(jnp.logical_and(q >= t, t > 0))
            def _():
                z_copy(k, q, cut, False).wait_send()

    ret_all().wait_send()

    @pl.loop(0, T)
    def _(c):
        @pl.when(c > t)
        def _():
            rs_right(c, False).wait_send()

        @pl.when(c < t)
        def _():
            rs_left(c, False).wait_send()


def up_kernel(
    x_up,
    d_up,
    down_in,
    real_in,
    grad_up,
    grad_down,
    real_out,
    left,
    right,
    done,
    passed,
    small,
    sem_left,
    sem_in,
    sem_out,
    sem_down_in,
    sem_down_out,
    sem_small,
):
    steps, _, wide = right.shape
    tall = passed.shape[1]

    def columns(n):
        return pl.ds(n * wide, wide)

    def lines(n):
        return pl.ds(n * tall, tall)

    lefts = pltpu.make_async_copy(x_up, left, sem_left)
    ins = [
        pltpu.make_async_copy(d_up.at[:, columns(n)], right.at[n], sem_in.at[n])
        for n in range(steps)
    ]
    outs = [
        pltpu.make_async_copy(done.at[n], grad_up.at[:, columns(n)], sem_out.at[n])
        for n in range(steps)
    ]
    down_ins = [
        pltpu.make_async_copy(down_in.at[lines(n)], passed.at[n], sem_down_in.at[n])
        for n in range(steps)
    ]
    down_outs = [
        pltpu.make_async_copy(passed.at[n], grad_down.at[lines(n)], sem_down_out.at[n])
        for n in range(steps)
    ]
    small_in = pltpu.make_async_copy(real_in, small, sem_small.at[0])
    small_out = pltpu.make_async_copy(small, real_out, sem_small.at[1])
    lefts.start()
    for n in range(steps):
        ins[n].start()
    small_in.start()
    for n in range(steps):
        down_ins[n].start()
    lefts.wait()
    for n in range(steps):
        ins[n].wait()
        done[n] = dot32(left[...], right[n]).astype(BF16)
        outs[n].start()
        down_ins[n].wait()
        down_outs[n].start()
    small_in.wait()
    small_out.start()
    for n in range(steps):
        outs[n].wait()
        down_outs[n].wait()
    small_out.wait()


def on_device(
    x_real,
    routes_real,
    gates_real,
    up_real,
    down_real,
    x_fake,
    routes_fake,
    gates_fake,
    cotangent,
    up_fake,
    down_fake,
):
    E = lax.axis_size("expert")
    T = lax.axis_size("tensor")
    tokens, part = x_real.shape
    top = routes_real.shape[1]
    cap = tokens // 2
    total = E * cap
    D = up_real.shape[1]
    FF = up_real.shape[2]
    NT = min(512, FF)
    half = T // 2
    vmem = pl.BlockSpec(memory_space=pltpu.VMEM)
    hbm = pl.BlockSpec(memory_space=pl.ANY)
    dma = pltpu.SemaphoreType.DMA
    real_out, x_up, d_up, grad_down = pl.pallas_call(
        functools.partial(moe_kernel, E, T),
        name="moe",
        out_shape=(
            jax.ShapeDtypeStruct((tokens, part), BF16),
            jax.ShapeDtypeStruct((D // 2, 2 * total), BF16),
            jax.ShapeDtypeStruct((2 * total, FF), BF16),
            jax.ShapeDtypeStruct((FF, D // 2), BF16),
        ),
        in_specs=[vmem] * 4 + [hbm] * 7,
        out_specs=(vmem, hbm, hbm, hbm),
        scratch_shapes=[
            pltpu.VMEM((3 * T, tokens, part), BF16),
            pltpu.VMEM((3 * T, total - cap, part), BF16),
            pltpu.VMEM((3 * T, total, part), BF16),
            pltpu.VMEM((total, FF), F32),
            pltpu.VMEM((total, FF), F32),
            pltpu.VMEM((D, FF), BF16),
            pltpu.VMEM((FF, D), BF16),
            pltpu.VMEM((2, total, tokens), BF16),
            pltpu.VMEM((top, total, tokens), BF16),
            pltpu.VMEM((3, total, 1), F32),
            pltpu.VMEM((2 * total, FF), BF16),
            pltpu.VMEM((total, FF), BF16),
            pltpu.VMEM((T, part, total), BF16),
            pltpu.VMEM((half, total, part), BF16),
            pltpu.VMEM((T, total, part), BF16),
            pltpu.VMEM((T, total, part), BF16),
            pltpu.VMEM((T, total, part), BF16),
            pltpu.VMEM((total, part), F32),
            pltpu.VMEM((total, part), BF16),
            pltpu.VMEM((total, part), BF16),
            pltpu.VMEM((FF // NT, NT, part), BF16),
            dma((3,)),
            dma((4,)),
            dma((3 * T, CUTS)),
            dma((3 * T, CUTS)),
            dma((3 * T, CUTS)),
            dma((3 * T,)),
            dma((3 * T,)),
            dma((half,)),
            dma((half,)),
            dma((half,)),
            dma((half,)),
            dma((half,)),
            dma((2,)),
            dma((FF // NT,)),
            dma((FF // NT,)),
            dma((FF // NT,)),
            dma((T,)),
            dma((T,)),
            dma((T,)),
            dma((T,)),
            dma((2,)),
            dma((FF // NT,)),
        ],
        compiler_params=pltpu.CompilerParams(
            collective_id=0, has_side_effects=True, vmem_limit_bytes=67043328
        ),
    )(
        routes_real.T,
        gates_real.T,
        routes_fake.T,
        gates_fake.T,
        x_real,
        x_fake,
        cotangent,
        up_real,
        down_real,
        up_fake,
        down_fake,
    )
    steps = 4
    wide = FF // steps
    grad_up, grad_down, real_out = pl.pallas_call(
        up_kernel,
        name="finish",
        out_shape=(
            jax.ShapeDtypeStruct((D // 2, FF), BF16),
            jax.ShapeDtypeStruct((FF, D // 2), BF16),
            jax.ShapeDtypeStruct((tokens, part), BF16),
        ),
        in_specs=[hbm] * 4,
        out_specs=(hbm,) * 3,
        scratch_shapes=[
            pltpu.VMEM((D // 2, 2 * total), BF16),
            pltpu.VMEM((steps, 2 * total, wide), BF16),
            pltpu.VMEM((steps, D // 2, wide), BF16),
            pltpu.VMEM((steps, wide, D // 2), BF16),
            pltpu.VMEM((tokens, part), BF16),
            dma(()),
            dma((steps,)),
            dma((steps,)),
            dma((steps,)),
            dma((steps,)),
            dma((2,)),
        ],
        compiler_params=pltpu.CompilerParams(vmem_limit_bytes=67043328),
    )(x_up, d_up, grad_down, real_out)
    return real_out, grad_up[None], grad_down[None]


def solution(mesh):
    in_specs = (
        P(("expert", "dp"), "tensor"),
        P(("expert", "dp"), None),
        P(("expert", "dp"), None),
        P("expert", None, "tensor"),
        P("expert", "tensor", None),
        P(("expert", "dp"), "tensor"),
        P(("expert", "dp"), None),
        P(("expert", "dp"), None),
        P(("expert", "dp"), "tensor"),
        P("expert", None, "tensor"),
        P("expert", "tensor", None),
    )
    out_specs = (
        P(("expert", "dp"), "tensor"),
        P("expert", "dp", "tensor"),
        P("expert", "tensor", "dp"),
    )
    return jax.shard_map(
        on_device, mesh=mesh, in_specs=in_specs, out_specs=out_specs, check_vma=False
    )
```

```python
import functools

import jax
import jax.numpy as jnp
from jax import lax
from jax.experimental import pallas as pl
from jax.experimental.pallas import tpu as pltpu
from jax.sharding import PartitionSpec as P

slope_const = 0.7978845608028654
cubic_coef = 0.044715
MESH = pl.DeviceIdType.MESH
F32 = jnp.float32
BF16 = jnp.bfloat16
LAG = 3
CUTS = 2


def dot32(left, right, dims=((1,), (0,))):
    return lax.dot_general(left, right, (dims, ((), ())), preferred_element_type=F32)


def tanh_of(value):
    return jnp.tanh(slope_const * (value + cubic_coef * value * value * value))


def gelu_from(value, inner):
    return 0.5 * value * (1.0 + inner)


def slope_from(value, inner):
    return 0.5 * (1.0 + inner) + 0.5 * value * (1.0 - inner * inner) * slope_const * (
        1.0 + 3.0 * cubic_coef * value * value
    )


def moe_kernel(
    experts,
    tensors,
    routes_real,
    gates_real,
    routes_fake,
    gates_fake,
    x_real,
    x_fake,
    cotangent,
    up_real,
    down_real,
    up_fake,
    down_fake,
    real_out,
    x_up,
    d_up,
    grad_down,
    whole,
    sendbuf,
    rows,
    acc0,
    acc1,
    weight0,
    weight1,
    pick,
    pick_k,
    gate,
    act,
    dpre,
    x_turned,
    other_d,
    partial,
    from_left,
    from_right,
    final,
    ret_send,
    returned,
    stage_down,
    final_out,
    in_sem,
    out_sem,
    w_sem,
    z_recv,
    z_right,
    z_left,
    x_send,
    x_recv,
    xt_keep,
    xt_send,
    xt_recv,
    d_send,
    d_recv,
    act_sems,
    dp_keep,
    dp_send,
    dp_recv,
    rsr_send,
    rsr_recv,
    rsl_send,
    rsl_recv,
    ret_sems,
    down_sem,
):
    E, T = experts, tensors
    top, tokens = routes_real.shape
    cap = tokens // 2
    total = E * cap
    part = x_real.shape[1]
    FF = act.shape[1]
    NT = stage_down.shape[1]
    tiles = FF // NT
    half = T // 2
    e = lax.axis_index("expert")
    t = lax.axis_index("tensor")
    d = lax.axis_index("dp")
    last = T - 1

    barrier = pltpu.get_barrier_semaphore()
    for s in range(1, E):
        pl.semaphore_signal(barrier, inc=1, device_id={"expert": e ^ s}, device_id_type=MESH)
    pl.semaphore_signal(barrier, inc=1, device_id={"dp": 1 - d}, device_id_type=MESH)

    @pl.when(t > 0)
    def _():
        pl.semaphore_signal(barrier, inc=1, device_id={"tensor": t - 1}, device_id_type=MESH)

    @pl.when(t < last)
    def _():
        pl.semaphore_signal(barrier, inc=1, device_id={"tensor": t + 1}, device_id_type=MESH)

    own_in = [
        pltpu.make_async_copy(src, whole.at[a * T + t], in_sem.at[a])
        for a, src in enumerate((x_real, x_fake, cotangent))
    ]
    for copy in own_in:
        copy.start()

    def load(src, dst, k):
        return pltpu.make_async_copy(src.at[0], dst, w_sem.at[k])

    square = (tokens, tokens)
    down_at = lax.broadcasted_iota(jnp.int32, square, 0)
    along = lax.broadcasted_iota(jnp.int32, square, 1)
    eye = down_at == along
    upper = (down_at < along).astype(BF16)
    labels_high = max(8, E)
    labels = lax.broadcasted_iota(jnp.int32, (labels_high, tokens), 0).astype(F32)
    slot_rows = lax.broadcasted_iota(jnp.int32, (total, tokens), 0).astype(F32)

    def stand_up(row):
        return jnp.sum(jnp.where(eye, row, 0.0), axis=1, keepdims=True)

    def positions(routes):
        names = [routes[k : k + 1, :].astype(F32) for k in range(top)]
        places = [(routes[k : k + 1, :] ^ e).astype(F32) for k in range(top)]
        hits = jnp.zeros((labels_high, tokens), F32)
        for name in names:
            hits = hits + (labels == name).astype(F32)
        before = dot32(hits.astype(BF16), upper)
        found = []
        for name, place in zip(names, places):
            slot = jnp.sum(jnp.where(labels == name, before, 0.0), axis=0, keepdims=True)
            found.append(place * cap + slot)
        return found

    chosen = jnp.zeros((total, tokens), BF16)
    for k, where in enumerate(positions(routes_real)):
        mask = (slot_rows == where).astype(F32).astype(BF16)
        pick_k[k] = mask
        chosen = chosen + mask
    pick[0] = chosen
    gate[0] = jnp.ones((total, 1), F32)
    for copy in own_in:
        copy.wait()

    pl.semaphore_wait(barrier, E + jnp.minimum(t, 1) + jnp.minimum(last - t, 1))

    piece = tokens // CUTS

    def z_copy(i, q, cut, right):
        k = (i // T) * T + q
        return pltpu.make_async_remote_copy(
            src_ref=whole.at[k, pl.ds(cut * piece, piece)],
            dst_ref=whole.at[k, pl.ds(cut * piece, piece)],
            send_sem=(z_right if right else z_left).at[k, cut],
            recv_sem=z_recv.at[k, cut],
            device_id={"tensor": t + 1 if right else t - 1},
            device_id_type=MESH,
        )

    near = jnp.minimum(t, last - t)

    def source(p, a):
        step = (p + 1) // 2
        side = jnp.where(jnp.logical_xor(t < half, a == 0), -1, 1)
        close = t + jnp.where(p % 2 == 1, side, -side) * step
        beyond = jnp.where(t < last - t, t + p - near, t - p + near)
        return jnp.where(p <= 2 * near, close, beyond)

    at_end = jnp.logical_or(t == 0, t == last)

    def send_own(i):
        for cut in range(CUTS):

            @pl.when(t < last)
            def _():
                z_copy(i, t, cut, True).start()

            @pl.when(t > 0)
            def _():
                z_copy(i, t, cut, False).start()

    def gather_step(i):
        q = source(i % T, i // T)

        @pl.when(jnp.logical_and(q == t, jnp.logical_not(at_end)))
        def _():
            send_own(i)

        for cut in range(CUTS):

            @pl.when(q != t)
            def _():
                z_copy(i, q, cut, True).wait_recv()

            @pl.when(jnp.logical_and(q < t, t < last))
            def _():
                z_copy(i, q, cut, True).start()

            @pl.when(jnp.logical_and(q > t, t > 0))
            def _():
                z_copy(i, q, cut, False).start()

    def x_copies(k):
        return [
            pltpu.make_async_remote_copy(
                src_ref=sendbuf.at[k, pl.ds((s - 1) * cap, cap)],
                dst_ref=rows.at[k, pl.ds(s * cap, cap)],
                send_sem=x_send.at[k],
                recv_sem=x_recv.at[k],
                device_id={"expert": e ^ s},
                device_id_type=MESH,
            )
            for s in range(1, E)
        ]

    def x_all(k):
        return pltpu.make_async_remote_copy(
            src_ref=sendbuf.at[k],
            dst_ref=rows.at[k, pl.ds(cap, total - cap)],
            send_sem=x_send.at[k],
            recv_sem=x_recv.at[k],
            device_id={"expert": e ^ 1},
            device_id_type=MESH,
        )

    def dispatch_step(i):
        a = i // T
        k = a * T + source(i % T, a)
        which = jnp.minimum(a, 1)
        picked = (dot32(pick[which], whole[k]) * gate[a]).astype(BF16)
        rows[k, 0:cap] = picked[0:cap]
        sendbuf[k] = picked[cap:total]
        for copy in x_copies(k):
            copy.start()

    inner = jnp.logical_not(at_end)

    def feed(i):
        @pl.when(at_end)
        def _():
            gather_step(i)

        dispatch_step(i)

    send_own(0)

    @pl.when(at_end)
    def _():
        send_own(T)
        send_own(2 * T)

    load(up_real, weight0, 0).start()

    dispatch_step(0)
    gate[1] = jnp.ones((total, 1), F32)
    chosen = jnp.zeros((total, tokens), BF16)
    gated = jnp.zeros((total, tokens), F32)
    for k, where in enumerate(positions(routes_fake)):
        mask = slot_rows == where
        chosen = chosen + mask.astype(F32).astype(BF16)
        gated = jnp.where(mask, gates_fake[k : k + 1, :], gated)
    pick[1] = chosen
    gate[2] = jnp.sum(gated, axis=1, keepdims=True)
    for i in range(1, LAG):
        gather_step(jnp.int32(i))
        dispatch_step(jnp.int32(i))

    @pl.when(inner)
    def _():
        gather_step(jnp.int32(LAG))


    def tile_at(n):
        return pl.ds(pl.multiple_of(n * NT, NT), NT)

    def part_at(q):
        return pl.ds(pl.multiple_of(q * part, part), part)

    def clear(target):
        @pl.loop(0, tiles)
        def _(n):
            target[:, tile_at(n)] = jnp.zeros((total, NT), F32)

    clear(acc0)
    load(down_real, weight1, 1).start()
    load(up_real, weight0, 0).wait()

    @pl.loop(0, T)
    def _(p):
        q = source(p, 0)
        x_all(q).wait_recv()

        @pl.loop(0, tiles)
        def _(n):
            acc0[:, tile_at(n)] += dot32(rows[q], weight0[part_at(q), tile_at(n)])

        feed(p + LAG)

        @pl.when(inner)
        def _():
            gather_step(p + LAG + 1)

    load(up_fake, weight0, 2).start()

    @pl.loop(0, tiles)
    def _(n):
        value = acc0[:, tile_at(n)]
        dpre[:, tile_at(n)] = gelu_from(value, tanh_of(value)).astype(BF16)

    def rs_right(c, first):
        return pltpu.make_async_remote_copy(
            src_ref=partial.at[c] if first else from_left.at[c],
            dst_ref=from_left.at[c],
            send_sem=rsr_send.at[c],
            recv_sem=rsr_recv.at[c],
            device_id={"tensor": t + 1},
            device_id_type=MESH,
        )

    def rs_left(c, first):
        return pltpu.make_async_remote_copy(
            src_ref=partial.at[c] if first else from_right.at[c],
            dst_ref=from_right.at[c],
            send_sem=rsl_send.at[c],
            recv_sem=rsl_recv.at[c],
            device_id={"tensor": t - 1},
            device_id_type=MESH,
        )

    def rs_round(h):
        c_right = last - h + t
        go_right = jnp.logical_and(h >= t, t < last)

        @pl.when(jnp.logical_and(go_right, t == 0))
        def _():
            rs_right(c_right, True).start()

        @pl.when(jnp.logical_and(go_right, t > 0))
        def _():
            rs_right(c_right, False).wait_recv()
            joined = from_left[c_right].astype(F32) + partial[c_right].astype(F32)
            from_left[c_right] = joined.astype(BF16)
            rs_right(c_right, False).start()

        c_left = h - (last - t)
        go_left = jnp.logical_and(h >= last - t, t > 0)

        @pl.when(jnp.logical_and(go_left, t == last))
        def _():
            rs_left(c_left, True).start()

        @pl.when(jnp.logical_and(go_left, t < last))
        def _():
            rs_left(c_left, False).wait_recv()
            joined = from_right[c_left].astype(F32) + partial[c_left].astype(F32)
            from_right[c_left] = joined.astype(BF16)
            rs_left(c_left, False).start()

    def ret_copies():
        return [
            pltpu.make_async_remote_copy(
                src_ref=ret_send.at[pl.ds(s * cap, cap)],
                dst_ref=returned.at[pl.ds(s * cap, cap)],
                send_sem=ret_sems.at[0],
                recv_sem=ret_sems.at[1],
                device_id={"expert": e ^ s},
                device_id_type=MESH,
            )
            for s in range(1, E)
        ]

    def ret_all():
        return pltpu.make_async_remote_copy(
            src_ref=ret_send.at[pl.ds(cap, total - cap)],
            dst_ref=returned.at[pl.ds(cap, total - cap)],
            send_sem=ret_sems.at[0],
            recv_sem=ret_sems.at[1],
            device_id={"expert": e ^ 1},
            device_id_type=MESH,
        )

    def rs_final():
        final[...] = partial[t].astype(F32)

        @pl.when(t > 0)
        def _():
            rs_right(t, False).wait_recv()
            final[...] += from_left[t].astype(F32)

        @pl.when(t < last)
        def _():
            rs_left(t, False).wait_recv()
            final[...] += from_right[t].astype(F32)

        summed = final[...].astype(BF16)
        ret_send[...] = summed
        returned[0:cap] = summed[0:cap]
        for copy in ret_copies():
            copy.start()

    def rs_slot(j):
        h = j // 2

        @pl.when(jnp.logical_and(j % 2 == 0, jnp.logical_and(j > 0, h < last)))
        def _():
            rs_round(h)

        @pl.when(j == 2 * last)
        def _():
            rs_final()

    load(down_real, weight1, 1).wait()

    @pl.loop(0, T)
    def _(k):
        c = jnp.where(t < half, last - k, k)
        partial[c] = dot32(dpre[...], weight1[:, part_at(c)]).astype(BF16)

        @pl.when(k == 0)
        def _():
            rs_round(jnp.int32(0))

        @pl.when(jnp.logical_and(inner, k < 2))
        def _():
            gather_step(T + LAG + 1 + k)

    load(down_fake, weight1, 3).start()

    def half_of(q):
        return q // half

    base = d * half

    def swap(q):
        other = q - (1 - d) * half
        return pltpu.make_async_remote_copy(
            src_ref=rows.at[2 * T + q],
            dst_ref=other_d.at[other],
            send_sem=d_send.at[other],
            recv_sem=d_recv.at[other],
            device_id={"dp": 1 - d},
            device_id_type=MESH,
        )

    def swap_in(j):
        return pltpu.make_async_remote_copy(
            src_ref=rows.at[2 * T + j],
            dst_ref=other_d.at[j],
            send_sem=d_send.at[j],
            recv_sem=d_recv.at[j],
            device_id={"dp": 1 - d},
            device_id_type=MESH,
        )

    def turned_keep(q):
        return pltpu.make_async_copy(
            x_turned.at[q],
            x_up.at[pl.ds((q - base) * part, part), pl.ds(0, total)],
            xt_keep.at[q - base],
        )

    def turned_send(q):
        other = q - (1 - d) * half
        return pltpu.make_async_remote_copy(
            src_ref=x_turned.at[q],
            dst_ref=x_up.at[pl.ds(other * part, part), pl.ds(total, total)],
            send_sem=xt_send.at[other],
            recv_sem=xt_recv.at[other],
            device_id={"dp": 1 - d},
            device_id_type=MESH,
        )

    def turned_in(j):
        return pltpu.make_async_remote_copy(
            src_ref=x_turned.at[j],
            dst_ref=x_up.at[pl.ds(j * part, part), pl.ds(total, total)],
            send_sem=xt_send.at[j],
            recv_sem=xt_recv.at[j],
            device_id={"dp": 1 - d},
            device_id_type=MESH,
        )

    clear(acc1)
    load(up_fake, weight0, 2).wait()

    @pl.loop(0, T)
    def _(p):
        q = source(p, 1)
        x_all(T + q).wait_recv()

        @pl.loop(0, tiles)
        def _(n):
            acc1[:, tile_at(n)] += dot32(rows[T + q], weight0[part_at(q), tile_at(n)])

        feed(T + p + LAG)
        rs_slot(p)

        @pl.when(jnp.logical_and(inner, p + LAG + 3 < 2 * T))
        def _():
            gather_step(T + p + LAG + 3)

        x_turned[q] = rows[T + q].T

        @pl.when(half_of(q) == d)
        def _():
            turned_keep(q).start()

        @pl.when(half_of(q) != d)
        def _():
            turned_send(q).start()

    @pl.loop(0, tiles)
    def _(n):
        value = acc1[:, tile_at(n)]
        inner = tanh_of(value)
        act[0:total, tile_at(n)] = gelu_from(value, inner).astype(BF16)
        acc1[:, tile_at(n)] = slope_from(value, inner)

    def act_across():
        return pltpu.make_async_remote_copy(
            src_ref=act.at[pl.ds(0, total)],
            dst_ref=act.at[pl.ds(total, total)],
            send_sem=act_sems.at[0],
            recv_sem=act_sems.at[1],
            device_id={"dp": 1 - d},
            device_id_type=MESH,
        )

    def dpre_keep(n):
        return pltpu.make_async_copy(
            dpre.at[:, tile_at(n)], d_up.at[n, pl.ds(0, total)], dp_keep.at[n]
        )

    def dpre_across(n):
        return pltpu.make_async_remote_copy(
            src_ref=dpre.at[:, tile_at(n)],
            dst_ref=d_up.at[n, pl.ds(total, total)],
            send_sem=dp_send.at[n],
            recv_sem=dp_recv.at[n],
            device_id={"dp": 1 - d},
            device_id_type=MESH,
        )

    def put_down(j, n):
        return pltpu.make_async_copy(
            stage_down.at[n], grad_down.at[tile_at(n), part_at(j)], down_sem.at[n]
        )

    first_down = jnp.clip(t, base, base + half - 1)

    def down_step(q):
        @pl.when(half_of(q) == d)
        def _():
            j = q - base
            swap_in(j).wait_recv()

            @pl.loop(0, tiles)
            def _(n):
                @pl.when(q != first_down)
                def _():
                    put_down(j, n).wait()

                tile = dot32(act[0:total, tile_at(n)], rows[2 * T + q], ((0,), (0,)))
                tile = tile + dot32(
                    act[total : 2 * total, tile_at(n)], other_d[j], ((0,), (0,))
                )
                stage_down[n] = tile.astype(BF16)
                put_down(j, n).start()

    clear(acc0)
    act_across().start()
    load(down_fake, weight1, 3).wait()

    def take_rows(q):
        x_all(2 * T + q).wait_recv()

        @pl.when(half_of(q) != d)
        def _():
            swap(q).start()

    @pl.loop(0, last)
    def _(p):
        q = source(p, 2)
        take_rows(q)

        @pl.loop(0, tiles)
        def _(n):
            acc0[:, tile_at(n)] += dot32(
                rows[2 * T + q], weight1[tile_at(n), part_at(q)], ((1,), (1,))
            )

        @pl.when(p + LAG < T)
        def _():
            feed(2 * T + p + LAG)

        @pl.when(jnp.logical_and(inner, p + LAG + 3 < T))
        def _():
            gather_step(2 * T + p + LAG + 3)

        rs_slot(T + p)

        @pl.when(p == 0)
        def _():
            act_across().wait_recv()

        @pl.when(p > 0)
        def _():
            down_step(source(p - 1, 2))

    q_last = source(last, 2)
    take_rows(q_last)

    @pl.loop(0, tiles)
    def _(n):
        back = acc0[:, tile_at(n)] + dot32(
            rows[2 * T + q_last], weight1[tile_at(n), part_at(q_last)], ((1,), (1,))
        )
        dpre[:, tile_at(n)] = (back * acc1[:, tile_at(n)]).astype(BF16)
        dpre_across(n).start()
        dpre_keep(n).start()

    rs_slot(T + last)
    down_step(source(last - 1, 2))
    down_step(q_last)

    @pl.loop(0, 3 * T)
    def _(k):
        x_all(k).wait_send()
        q = k % T
        for cut in range(CUTS):

            @pl.when(jnp.logical_and(q <= t, t < last))
            def _():
                z_copy(k, q, cut, True).wait_send()

            @pl.when(jnp.logical_and(q >= t, t > 0))
            def _():
                z_copy(k, q, cut, False).wait_send()

    @pl.loop(0, T)
    def _(c):
        @pl.when(c > t)
        def _():
            rs_right(c, False).wait_send()

        @pl.when(c < t)
        def _():
            rs_left(c, False).wait_send()

    ret_all().wait_recv()
    out = jnp.zeros((tokens, part), F32)
    for k in range(top):
        back = dot32(pick_k[k], returned[...], ((0,), (0,)))
        out = out + stand_up(gates_real[k : k + 1, :]) * back
    final_out[...] = out.astype(BF16)
    out_copy = pltpu.make_async_copy(final_out, real_out, out_sem)
    out_copy.start()

    @pl.loop(0, tiles)
    def _(n):
        put_down(0, n).wait()
        dpre_across(n).wait()
        dpre_keep(n).wait()

    @pl.loop(0, half)
    def _(j):
        turned_in(j).wait()
        turned_keep(base + j).wait()
        swap_in(j).wait_send()

    act_across().wait_send()

    ret_all().wait_send()
    out_copy.wait()


def up_kernel(
    x_up,
    d_up,
    down_in,
    real_in,
    grad_up,
    grad_down,
    real_out,
    left,
    right,
    done,
    passed,
    small,
    sem_left,
    sem_in,
    sem_out,
    sem_down_in,
    sem_down_out,
    sem_small,
):
    steps, _, wide = right.shape
    tall = passed.shape[1]

    def columns(n):
        return pl.ds(n * wide, wide)

    def lines(n):
        return pl.ds(n * tall, tall)

    lefts = pltpu.make_async_copy(x_up, left, sem_left)
    ins = [
        pltpu.make_async_copy(d_up.at[n], right.at[n], sem_in.at[n])
        for n in range(steps)
    ]
    outs = [
        pltpu.make_async_copy(done.at[n], grad_up.at[:, columns(n)], sem_out.at[n])
        for n in range(steps)
    ]
    down_ins = [
        pltpu.make_async_copy(down_in.at[lines(n)], passed.at[n], sem_down_in.at[n])
        for n in range(steps)
    ]
    down_outs = [
        pltpu.make_async_copy(passed.at[n], grad_down.at[lines(n)], sem_down_out.at[n])
        for n in range(steps)
    ]
    small_in = pltpu.make_async_copy(real_in, small, sem_small.at[0])
    small_out = pltpu.make_async_copy(small, real_out, sem_small.at[1])
    lefts.start()
    small_in.start()
    for n in range(steps):
        ins[n].start()
    for n in range(steps):
        down_ins[n].start()
    lefts.wait()
    for n in range(steps):
        ins[n].wait()
        down_ins[n].wait()
        down_outs[n].start()
        for m in range(2):
            lines_up = pl.ds(m * (left.shape[0] // 2), left.shape[0] // 2)
            done[n, lines_up] = dot32(left[lines_up], right[n]).astype(BF16)
        outs[n].start()
    small_in.wait()
    small_out.start()
    for n in range(steps):
        outs[n].wait()
        down_outs[n].wait()
    small_out.wait()


def on_device(
    x_real,
    routes_real,
    gates_real,
    up_real,
    down_real,
    x_fake,
    routes_fake,
    gates_fake,
    cotangent,
    up_fake,
    down_fake,
):
    E = lax.axis_size("expert")
    T = lax.axis_size("tensor")
    tokens, part = x_real.shape
    top = routes_real.shape[1]
    cap = tokens // 2
    total = E * cap
    D = up_real.shape[1]
    FF = up_real.shape[2]
    NT = min(512, FF)
    half = T // 2
    vmem = pl.BlockSpec(memory_space=pltpu.VMEM)
    hbm = pl.BlockSpec(memory_space=pl.ANY)
    dma = pltpu.SemaphoreType.DMA
    real_out, x_up, d_up, grad_down = pl.pallas_call(
        functools.partial(moe_kernel, E, T),
        name="moe",
        out_shape=(
            jax.ShapeDtypeStruct((tokens, part), BF16),
            jax.ShapeDtypeStruct((D // 2, 2 * total), BF16),
            jax.ShapeDtypeStruct((FF // NT, 2 * total, NT), BF16),
            jax.ShapeDtypeStruct((FF, D // 2), BF16),
        ),
        in_specs=[vmem] * 4 + [hbm] * 7,
        out_specs=(hbm,) * 4,
        scratch_shapes=[
            pltpu.VMEM((3 * T, tokens, part), BF16),
            pltpu.VMEM((3 * T, total - cap, part), BF16),
            pltpu.VMEM((3 * T, total, part), BF16),
            pltpu.VMEM((total, FF), F32),
            pltpu.VMEM((total, FF), F32),
            pltpu.VMEM((D, FF), BF16),
            pltpu.VMEM((FF, D), BF16),
            pltpu.VMEM((2, total, tokens), BF16),
            pltpu.VMEM((top, total, tokens), BF16),
            pltpu.VMEM((3, total, 1), F32),
            pltpu.VMEM((2 * total, FF), BF16),
            pltpu.VMEM((total, FF), BF16),
            pltpu.VMEM((T, part, total), BF16),
            pltpu.VMEM((half, total, part), BF16),
            pltpu.VMEM((T, total, part), BF16),
            pltpu.VMEM((T, total, part), BF16),
            pltpu.VMEM((T, total, part), BF16),
            pltpu.VMEM((total, part), F32),
            pltpu.VMEM((total, part), BF16),
            pltpu.VMEM((total, part), BF16),
            pltpu.VMEM((FF // NT, NT, part), BF16),
            pltpu.VMEM((tokens, part), BF16),
            dma((3,)),
            dma(()),
            dma((4,)),
            dma((3 * T, CUTS)),
            dma((3 * T, CUTS)),
            dma((3 * T, CUTS)),
            dma((3 * T,)),
            dma((3 * T,)),
            dma((half,)),
            dma((half,)),
            dma((half,)),
            dma((half,)),
            dma((half,)),
            dma((2,)),
            dma((FF // NT,)),
            dma((FF // NT,)),
            dma((FF // NT,)),
            dma((T,)),
            dma((T,)),
            dma((T,)),
            dma((T,)),
            dma((2,)),
            dma((FF // NT,)),
        ],
        compiler_params=pltpu.CompilerParams(
            collective_id=0, has_side_effects=True, vmem_limit_bytes=67043328
        ),
    )(
        routes_real.T,
        gates_real.T,
        routes_fake.T,
        gates_fake.T,
        x_real,
        x_fake,
        cotangent,
        up_real,
        down_real,
        up_fake,
        down_fake,
    )
    steps = FF // NT
    wide = NT
    grad_up, grad_down, real_out = pl.pallas_call(
        up_kernel,
        name="finish",
        out_shape=(
            jax.ShapeDtypeStruct((D // 2, FF), BF16),
            jax.ShapeDtypeStruct((FF, D // 2), BF16),
            jax.ShapeDtypeStruct((tokens, part), BF16),
        ),
        in_specs=[hbm] * 4,
        out_specs=(hbm,) * 3,
        scratch_shapes=[
            pltpu.VMEM((D // 2, 2 * total), BF16),
            pltpu.VMEM((steps, 2 * total, wide), BF16),
            pltpu.VMEM((steps, D // 2, wide), BF16),
            pltpu.VMEM((steps, wide, D // 2), BF16),
            pltpu.VMEM((tokens, part), BF16),
            dma(()),
            dma((steps,)),
            dma((steps,)),
            dma((steps,)),
            dma((steps,)),
            dma((2,)),
        ],
        compiler_params=pltpu.CompilerParams(vmem_limit_bytes=67043328),
    )(x_up, d_up, grad_down, real_out)
    return real_out, grad_up[None], grad_down[None]


def solution(mesh):
    in_specs = (
        P(("expert", "dp"), "tensor"),
        P(("expert", "dp"), None),
        P(("expert", "dp"), None),
        P("expert", None, "tensor"),
        P("expert", "tensor", None),
        P(("expert", "dp"), "tensor"),
        P(("expert", "dp"), None),
        P(("expert", "dp"), None),
        P(("expert", "dp"), "tensor"),
        P("expert", None, "tensor"),
        P("expert", "tensor", None),
    )
    out_specs = (
        P(("expert", "dp"), "tensor"),
        P("expert", "dp", "tensor"),
        P("expert", "tensor", "dp"),
    )
    return jax.shard_map(
        on_device, mesh=mesh, in_specs=in_specs, out_specs=out_specs, check_vma=False
    )
```
